32 devices in a mesh: row: 8 (over y, x, core), col: 4 (over z).
Axes of the slice: x: 2, y: 2, z: 4, core: 2. Of those that a mesh axis runs over, the one named last changes fastest.
Arguments:
- species: float32 [2, 256, 256, 128], P(None, None, 'row', 'col'), may hold values from -6 to 6
- coupling: float32 [2, 2], replicated, may hold values from -4 to 4
- symbol_x: float32 [256], replicated, may hold values from 0.3 to 3
- symbol_y: float32 [256], replicated, may hold values from 0.3 to 3
- symbol_z: float32 [128], replicated, may hold values from 0.3 to 3
Outputs:
- modes: float32 [2, 256, 256, 128], P(None, 'row', 'col')
The draws below stay inside these ranges and needn't reach their ends.
All inputs are finite; a program needn't handle non-finite values.
Results may differ from the reference program's by a relative error of at most 0.000078.
Values sent between devices are 32-bit elements.
No kernel may reach another device: no remote copies, remote signals or barrier semaphores. Data moves between devices by JAX's collectives and lax.ppermute only.
A program may use at most 128 MiB of HBM per device.

```python
import jax
import jax.numpy as jnp
from jax import lax

GRID_X = 256
GRID_Y = 256
GRID_Z = 128
FIELDS = 2


def block_scale(own_key, shape, cuts, low, top_value):
    level, own = 1.0, jax.random.fold_in(own_key, 6)
    for position, shards_of in cuts:
        draws = jnp.exp(jax.random.uniform(jax.random.fold_in(own, position), (shards_of,), jnp.float32, low / len(cuts), top_value / len(cuts)))
        level = level * jnp.repeat(draws, shape[position] // shards_of).reshape([-1 if axis == position else 1 for axis in range(len(shape))])
    return level


def scatter_about(key, extent, width, limit, shards=(), kind=jnp.bfloat16):
    values = width * jax.random.normal(key, extent, jnp.float32)
    if shards:
        values = values * block_scale(key, extent, shards, -0.22, 0.18)
    return jnp.clip(values, -limit, limit).astype(kind)


def setup_inputs(seed: int = 0) -> dict:
    seeds = jax.random.split(jax.random.key(seed), 6)
    species = scatter_about(seeds[0], (FIELDS, GRID_X, GRID_Y, GRID_Z), 1.0, 6.0, ((2, 8), (3, 4)), jnp.float32)
    coupling = scatter_about(seeds[1], (FIELDS, FIELDS), 0.7, 4.0, (), jnp.float32)
    symbol_x = jnp.clip(jax.random.uniform(seeds[2], (GRID_X,), jnp.float32, 0.3, 3.0), 0.3, 3.0)
    symbol_y = jnp.clip(jax.random.uniform(seeds[3], (GRID_Y,), jnp.float32, 0.3, 3.0), 0.3, 3.0)
    symbol_z = jnp.clip(jax.random.uniform(seeds[4], (GRID_Z,), jnp.float32, 0.3, 3.0), 0.3, 3.0)
    return {"species": species, "coupling": coupling, "symbol_x": symbol_x, "symbol_y": symbol_y, "symbol_z": symbol_z}


def mode_table(count):
    rank = jnp.arange(count)
    angle = (jnp.pi / (count + 1)) * (((rank[:, None] + 1) * (rank[None, :] + 1)) % (2 * count + 2)).astype(jnp.float32)
    return jnp.sin(angle) * (2.0 / (count + 1)) ** 0.5


def transform_dim(values, dim):
    moved = jnp.tensordot(values, mode_table(values.shape[dim]), axes=([dim], [0]), precision=lax.Precision.HIGHEST)
    return jnp.moveaxis(moved, -1, dim)


def reference(species, coupling, symbol_x, symbol_y, symbol_z):
    modes = species
    modes = transform_dim(modes, 1)
    modes = transform_dim(modes, 2)
    modes = transform_dim(modes, 3)
    symbol = symbol_x[:, None, None] + symbol_y[None, :, None] + symbol_z[None, None, :]
    weight_xyz = 1.0 / (1.0 + symbol)
    mixed_fields = jnp.einsum("ab,bxyz->axyz", coupling, modes, precision=lax.Precision.HIGHEST)
    modes = weight_xyz * modes + (1.0 - weight_xyz) * mixed_fields
    return modes
```

```python
import functools

import jax
import jax.numpy as jnp
import numpy as np
from jax import lax
from jax.experimental import pallas as pl
from jax.experimental.pallas import tpu as pltpu
from jax.sharding import PartitionSpec as P

LANES = 128
SUBLANES = 8
SHARES = (1, 3, 4)


ANY = pl.BlockSpec(memory_space=pl.ANY)
VMEM = pl.BlockSpec(memory_space=pltpu.VMEM)
SMEM = pl.BlockSpec(memory_space=pltpu.SMEM)


def mode_table(count):
    rank = np.arange(1, count + 1)
    angle = np.pi / (count + 1) * (rank[:, None] * rank[None, :] % (2 * count + 2))
    return np.sin(angle) * np.sqrt(2.0 / (count + 1))


def split_table(table):
    table = table.astype(np.float32)
    high = table.astype(jnp.bfloat16)
    low = (table - high.astype(np.float32)).astype(jnp.bfloat16)
    return high, low


def split(values):
    high = values.astype(jnp.bfloat16)
    low = (values - high.astype(jnp.float32)).astype(jnp.bfloat16)
    return high, low


def dot(a, b, contract):
    return lax.dot_general(
        a, b, ((contract[:1], contract[1:]), ((), ())), preferred_element_type=jnp.float32
    )


def block_transpose(tiles, width):
    count = len(tiles)
    lane = lax.broadcasted_iota(jnp.int32, tiles[0].shape, 1)
    step = count // 2
    while step:
        odd = (lane // (width * step)) % 2 == 1
        result = list(tiles)
        for g in range(count):
            if g & step:
                continue
            a, b = tiles[g], tiles[g + step]
            shift = width * step
            result[g] = jnp.where(odd, pltpu.roll(b, shift, 1), a)
            result[g + step] = jnp.where(odd, b, pltpu.roll(a, LANES - shift, 1))
        tiles = result
        step //= 2
    return tiles


def x_kernel(peers, units, groups, x_hbm, *refs):
    n_chunk = len(units)
    tables, refs = refs[:n_chunk], refs[n_chunk:]
    outs, refs = refs[: n_chunk * peers], refs[n_chunk * peers :]
    x_vmem, in_sems, out_sems = refs[:3]
    scratch, packed = refs[3 : 3 + n_chunk], refs[3 + n_chunk :]
    fields, rows, width = x_vmem.shape
    blocks = rows // LANES
    me = lax.axis_index("row")
    loads = [
        pltpu.make_async_copy(x_hbm.at[f], x_vmem.at[f], in_sems.at[f]) for f in range(fields)
    ]
    for load in loads:
        load.start()
    for f in range(fields):
        loads[f].wait()
        high, low = split(x_vmem[f])
        for q in range(n_chunk):
            table = tables[q][...]
            lines = table.shape[0] // 2
            both = dot(table, high, (1, 1))
            result = both[:lines] + both[lines:] + dot(table[:lines], low, (1, 1))
            for kx in range(lines // peers):
                for b in range(blocks):
                    scratch[q][kx, b * peers : (b + 1) * peers, :] = result[
                        kx * peers : (kx + 1) * peers, b * LANES : (b + 1) * LANES
                    ]
            for peer in range(peers):
                for hi in range(units[q]):
                    tiles = [
                        scratch[q][hi * groups + g, pl.ds(peer, blocks, stride=peers), :]
                        for g in range(groups)
                    ]
                    for t, tile in enumerate(block_transpose(tiles, LANES // groups)):
                        packed[q][
                            peer, f, t * blocks : (t + 1) * blocks, hi * LANES : (hi + 1) * LANES
                        ] = tile
    stores = []
    for q in range(n_chunk):
        for k in range(peers):
            stores.append(
                pltpu.make_async_copy(
                    packed[q].at[me ^ k], outs[q * peers + k], out_sems.at[q * peers + k]
                )
            )
            stores[-1].start()
    for store in stores:
        store.wait()


def y_kernel(peers, heads, *refs):
    ins, refs = refs[:peers], refs[peers:]
    table, refs = refs[0], refs[1:]
    outs, refs = refs[:heads], refs[heads:]
    gathered, result, in_sems, out_sems = refs
    fields, share = ins[0].shape[:2]
    out_share = outs[0].shape[1]
    row, col = lax.axis_index("row"), lax.axis_index("col")
    loads = []
    for k in range(peers):
        place = pl.ds(pl.multiple_of((row ^ k) * share, share), share)
        loads.append(pltpu.make_async_copy(ins[k], gathered.at[:, place, :], in_sems.at[k]))
        loads[-1].start()
    for load in loads:
        load.wait()
    for f in range(fields):
        high, low = split(gathered[f])
        result[f] = dot(table[...], jnp.concatenate([high, high, low], axis=0), (1, 0))
    stores = []
    for k in range(heads):
        place = pl.ds(pl.multiple_of((col ^ k) * out_share, out_share), out_share)
        stores.append(pltpu.make_async_copy(result.at[:, place, :], outs[k], out_sems.at[k]))
        stores[-1].start()
    for store in stores:
        store.wait()


def z_kernel(peers, groups, first, has_prior, *refs):
    ins, refs = refs[:peers], refs[peers:]
    table_high, table_low, syz, symbol_x, coupling = refs[:5]
    refs = refs[5 + has_prior :]
    modes, gathered, wide, mixed, in_sems, out_sem = refs
    _, fields, share, lanes = gathered.shape
    row, col = lax.axis_index("row"), lax.axis_index("col")
    loads = []
    for k in range(peers):
        loads.append(pltpu.make_async_copy(ins[k], gathered.at[col ^ k], in_sems.at[k]))
        loads[-1].start()
    depth, out_width = table_high.shape
    z_share = depth // peers
    wide[...] = jnp.zeros_like(wide)
    for part, table in enumerate((table_high, table_low, table_high)):
        for c in range(peers):
            for g in range(groups):
                start = (part * peers + c) * LANES + g * z_share
                wide[start : start + z_share, g * out_width : (g + 1) * out_width] = table[
                    c * z_share : (c + 1) * z_share, :
                ]
    for load in loads:
        load.wait()
    units = lanes // LANES
    lines = modes.shape[1] // 1
    del lines
    for hi in range(units):
        parts = []
        for f in range(fields):
            block = jnp.concatenate(
                [gathered[c, f, :, hi * LANES : (hi + 1) * LANES] for c in range(peers)], axis=1
            )
            high, low = split(block)
            parts.append(jnp.concatenate([high, high, low], axis=1))
        old = dot(jnp.concatenate(parts, axis=0), wide[...], (1, 0))
        for g in range(groups):
            kx = hi * groups + g
            line = row * (symbol_x.shape[0] // lax.axis_size("row")) + first + kx
            weight = 1.0 / (syz[...] + symbol_x[line])
            rest = 1.0 - weight
            mine = [
                old[f * share : (f + 1) * share, g * out_width : (g + 1) * out_width]
                for f in range(fields)
            ]
            for a in range(fields):
                mix = coupling[a, 0] * mine[0]
                for b in range(1, fields):
                    mix = mix + coupling[a, b] * mine[b]
                mixed[a, kx] = weight * mine[a] + rest * mix
    store = pltpu.make_async_copy(
        mixed, modes.at[:, pl.ds(first, units * groups)], out_sem
    )
    store.start()
    store.wait()


def solution(mesh):
    rows, cols = mesh.shape["row"], mesh.shape["col"]

    def exchange(arrays, axis):
        count = mesh.shape[axis]
        return [arrays[0]] + [
            lax.ppermute(arrays[k], axis, [(i, i ^ k) for i in range(count)])
            for k in range(1, count)
        ]

    def local(species, coupling, symbol_x, symbol_y, symbol_z):
        fields, size_x, share_y, share_z = species.shape
        size_y, size_z = share_y * rows, share_z * cols
        share_kx, share_ky = size_x // rows, size_y // cols
        groups = LANES // share_z
        blocks = share_y // groups
        all_units = share_kx // groups
        units = [all_units * s // sum(SHARES) for s in SHARES]
        assert sum(units) == all_units
        firsts = [groups * sum(units[:q]) for q in range(len(units))]
        f32 = jnp.float32

        lines = jnp.transpose(species, (0, 2, 3, 1)).reshape(fields, share_y * share_z, size_x)

        table_x = mode_table(size_x)

        def chunk_table(q):
            picked = [
                peer * share_kx + firsts[q] + kx
                for kx in range(units[q] * groups)
                for peer in range(rows)
            ]
            return jnp.asarray(np.concatenate(split_table(table_x[picked]), axis=0))

        def x_step(chunks):
            us = [units[q] for q in chunks]
            shapes = [
                jax.ShapeDtypeStruct((fields, share_y, u * LANES), f32)
                for u in us
                for _ in range(rows)
            ]
            return pl.pallas_call(
                functools.partial(x_kernel, rows, us, groups),
                out_shape=shapes,
                in_specs=[ANY] + [VMEM] * len(us),
                out_specs=[ANY] * len(shapes),
                scratch_shapes=[
                    pltpu.VMEM(lines.shape, f32),
                    pltpu.SemaphoreType.DMA((fields,)),
                    pltpu.SemaphoreType.DMA((len(shapes),)),
                ]
                + [pltpu.VMEM((u * groups, blocks * rows, LANES), f32) for u in us]
                + [pltpu.VMEM((rows, fields, share_y, u * LANES), f32) for u in us],
                cost_estimate=pl.CostEstimate(
                    flops=6 * lines.size * rows * groups * sum(us),
                    bytes_accessed=8 * lines.size,
                    transcendentals=0,
                ),
                name="x_step",
            )(lines, *[chunk_table(q) for q in chunks])

        order = [
            peer * share_y + b * groups + t
            for peer in range(rows)
            for t in range(groups)
            for b in range(blocks)
        ]
        high, low = split_table(mode_table(size_y)[:, order])
        table_y = jnp.asarray(np.concatenate([high, low, high], axis=1))

        def y_step(arrays):
            lanes = arrays[0].shape[2]
            shape = jax.ShapeDtypeStruct((fields, share_ky, lanes), f32)
            return pl.pallas_call(
                functools.partial(y_kernel, rows, cols),
                out_shape=[shape] * cols,
                in_specs=[ANY] * rows + [VMEM],
                out_specs=[ANY] * cols,
                scratch_shapes=[
                    pltpu.VMEM((fields, size_y, lanes), f32),
                    pltpu.VMEM((fields, size_y, lanes), f32),
                    pltpu.SemaphoreType.DMA((rows,)),
                    pltpu.SemaphoreType.DMA((cols,)),
                ],
                cost_estimate=pl.CostEstimate(
                    flops=6 * fields * size_y * size_y * lanes,
                    bytes_accessed=8 * fields * size_y * lanes,
                    transcendentals=0,
                ),
                name="y_step",
            )(*arrays, table_y)

        table_z = [jnp.asarray(t) for t in split_table(mode_table(size_z))]
        part_y = lax.dynamic_slice_in_dim(symbol_y, lax.axis_index("col") * share_ky, share_ky)
        syz = 1.0 + (part_y[:, None] + symbol_z[None, :])
        out_shape = jax.ShapeDtypeStruct((fields, share_kx, share_ky, size_z), f32)

        def z_step(q, arrays, prior):
            lanes = arrays[0].shape[2]
            has_prior = prior is not None
            return pl.pallas_call(
                functools.partial(z_kernel, cols, groups, firsts[q], has_prior),
                out_shape=out_shape,
                in_specs=[ANY] * cols + [VMEM] * 3 + [SMEM] * 2 + [ANY] * has_prior,
                out_specs=ANY,
                input_output_aliases={cols + 5: 0} if has_prior else {},
                scratch_shapes=[
                    pltpu.VMEM((cols, fields, share_ky, lanes), f32),
                    pltpu.VMEM((3 * cols * LANES, groups * size_z), jnp.bfloat16),
                    pltpu.VMEM((fields, units[q] * groups, share_ky, size_z), f32),
                    pltpu.SemaphoreType.DMA((cols,)),
                    pltpu.SemaphoreType.DMA,
                ],
                cost_estimate=pl.CostEstimate(
                    flops=6 * fields * share_ky * lanes * cols * groups * size_z,
                    bytes_accessed=8 * cols * fields * share_ky * lanes,
                    transcendentals=0,
                ),
                name="z_step",
            )(*arrays, *table_z, syz, symbol_x, coupling, *([prior] if has_prior else []))

        chunks = list(range(len(units)))
        sent = x_step(chunks[:1]) + x_step(chunks[1:])
        lines_y = [exchange(sent[q * rows : (q + 1) * rows], "row") for q in chunks]
        lines_z = [exchange(y_step(a), "col") for a in lines_y]
        modes = None
        for q in chunks:
            modes = z_step(q, lines_z[q], modes)
        return modes

    return jax.shard_map(
        local,
        mesh=mesh,
        in_specs=(P(None, None, "row", "col"), P(), P(), P(), P()),
        out_specs=P(None, "row", "col", None),
        check_vma=False,
    )
```

```python
import functools

import jax
import jax.numpy as jnp
import numpy as np
from jax import lax
from jax.experimental import pallas as pl
from jax.experimental.pallas import tpu as pltpu
from jax.sharding import PartitionSpec as P


LANES = 128
SPARE = 4 << 20
SHARES = (1, 2, 3, 2)


ANY = pl.BlockSpec(memory_space=pl.ANY)
VMEM = pl.BlockSpec(memory_space=pltpu.VMEM)
HBM = pl.BlockSpec(memory_space=pltpu.HBM)
SMEM = pl.BlockSpec(memory_space=pltpu.SMEM)


def mode_table(count):
    rank = np.arange(1, count + 1)
    angle = np.pi / (count + 1) * (rank[:, None] * rank[None, :] % (2 * count + 2))
    return np.sin(angle) * np.sqrt(2.0 / (count + 1))


def split_table(table):
    table = table.astype(np.float32)
    high = table.astype(jnp.bfloat16)
    low = (table - high.astype(np.float32)).astype(jnp.bfloat16)
    return high, low


def split(values):
    high = values.astype(jnp.bfloat16)
    low = (values - high.astype(jnp.float32)).astype(jnp.bfloat16)
    return high, low


def dot(a, b, contract):
    return lax.dot_general(
        a, b, ((contract[:1], contract[1:]), ((), ())), preferred_element_type=jnp.float32
    )


def block_transpose(tiles, width):
    count = len(tiles)
    lane = lax.broadcasted_iota(jnp.int32, tiles[0].shape, 1)
    step = count // 2
    while step:
        odd = (lane // (width * step)) % 2 == 1
        result = list(tiles)
        for g in range(count):
            if g & step:
                continue
            a, b = tiles[g], tiles[g + step]
            shift = width * step
            result[g] = jnp.where(odd, pltpu.roll(b, shift, 1), a)
            result[g + step] = jnp.where(odd, b, pltpu.roll(a, LANES - shift, 1))
        tiles = result
        step //= 2
    return tiles


def x_kernel(chips, units, groups, first, lines, table_ref, *refs):
    if not first:
        refs = refs[len(units) * chips :]
    outs, refs = refs[: len(units) * chips], refs[len(units) * chips :]
    scratch = refs[0]
    fields, rows, _ = lines.shape
    blocks = rows // LANES
    share_y = blocks * groups
    me = lax.axis_index("row")
    pair = me % 2
    owner = pair if first else 1 - pair
    if first:
        source, sems = refs[1:]
        loads = [
            pltpu.make_async_copy(lines.at[f], source.at[f], sems.at[f]) for f in range(fields)
        ]
        for load in loads:
            load.start()
    else:
        source = lines
    depth = table_ref.shape[0] // 2
    table = table_ref[pl.ds(pl.multiple_of(pair * depth, depth), depth), :]
    half = depth // 2
    tall = scratch.shape[2] // blocks
    for f in range(fields):
        if first:
            loads[f].wait()
        high, low = split(source[f])
        both = dot(table, high, (1, 1))
        result = both[:half] + both[half:] + dot(table[:half], low, (1, 1))
        for j in range(half // tall):
            for b in range(blocks):
                scratch[f, j, b * tall : (b + 1) * tall, :] = result[
                    j * tall : (j + 1) * tall, b * LANES : (b + 1) * LANES
                ]
        start = 0
        for q, count in enumerate(units):
            for k in range(chips):
                chip = (me // 2) ^ k
                for hi in range(count):
                    tiles = []
                    for g in range(groups):
                        at = (start + hi * groups + g) * chips
                        place = pl.ds(at % tall + chip, blocks, stride=tall)
                        tiles.append(scratch[f, at // tall, place, :])
                    for t, tile in enumerate(block_transpose(tiles, LANES // groups)):
                        place = pl.ds(
                            pl.multiple_of(owner * share_y + t * blocks, blocks), blocks
                        )
                        outs[q * chips + k][f, place, hi * LANES : (hi + 1) * LANES] = tile
            start += count * groups


def y_kernel(peers, heads, *refs):
    ins, refs = refs[:peers], refs[peers:]
    table, outs, gathered = refs[0], refs[1 : 1 + heads], refs[1 + heads]
    fields, share = ins[0].shape[:2]
    out_share = outs[0].shape[1]
    chip, col = lax.axis_index("row") // 2, lax.axis_index("col")
    left = jnp.concatenate(
        [
            table[pl.ds(pl.multiple_of((col ^ k) * out_share, out_share), out_share), :]
            for k in range(heads)
        ],
        axis=0,
    )
    for f in range(fields):
        for k in range(peers):
            place = pl.ds(pl.multiple_of((chip ^ k) * share, share), share)
            high, low = split(ins[k][f])
            gathered[f, 0, place, :] = high
            gathered[f, 1, place, :] = low
    for f in range(fields):
        high, low = gathered[f, 0], gathered[f, 1]
        result = dot(left, jnp.concatenate([high, high, low], axis=0), (1, 0))
        for k in range(heads):
            outs[k][f] = result[k * out_share : (k + 1) * out_share]


def z_table_kernel(peers, groups, table_high, table_low, wide):
    depth, out_width = table_high.shape
    z_share = depth // peers
    col = lax.axis_index("col")
    wide[...] = jnp.zeros_like(wide)
    for part, table in enumerate((table_high, table_low, table_high)):
        for k in range(peers):
            piece = table[pl.ds(pl.multiple_of((col ^ k) * z_share, z_share), z_share), :]
            for g in range(groups):
                start = (part * peers + k) * LANES + g * z_share
                wide[start : start + z_share, g * out_width : (g + 1) * out_width] = piece


def z_kernel(peers, groups, first, has_prior, *refs):
    ins, refs = refs[:peers], refs[peers:]
    wide, syz, symbol_x, coupling = refs[:4]
    modes, mixed, sems = refs[4 + has_prior :]
    fields, share, lanes = ins[0].shape
    units = lanes // LANES
    out_width = wide.shape[1] // groups
    row = lax.axis_index("row")
    parts = []
    for hi in range(units):
        for f in range(fields):
            block = jnp.concatenate(
                [ins[k][f, :, hi * LANES : (hi + 1) * LANES] for k in range(peers)], axis=1
            )
            high, low = split(block)
            parts.append(jnp.concatenate([high, high, low], axis=1))
    old = dot(jnp.concatenate(parts, axis=0), wide[...], (1, 0))
    stores = []
    for hi in range(units):
        for g in range(groups):
            kx = hi * groups + g
            line = row * (symbol_x.shape[0] // lax.axis_size("row")) + first + kx
            weight = 1.0 / (syz[...] + symbol_x[line])
            rest = 1.0 - weight
            mine = [
                old[
                    (hi * fields + f) * share : (hi * fields + f + 1) * share,
                    g * out_width : (g + 1) * out_width,
                ]
                for f in range(fields)
            ]
            for a in range(fields):
                mix = coupling[a, 0] * mine[0]
                for b in range(1, fields):
                    mix = mix + coupling[a, b] * mine[b]
                mixed[a, kx] = weight * mine[a] + rest * mix
        stores.append(
            pltpu.make_async_copy(
                mixed.at[:, hi * groups : (hi + 1) * groups],
                modes.at[:, pl.ds(first + hi * groups, groups)],
                sems.at[hi],
            )
        )
        stores[-1].start()
    for store in stores:
        store.wait()


def solution(mesh):
    rows, cols = mesh.shape["row"], mesh.shape["col"]
    n_chunk = len(SHARES)

    def exchange(arrays, axis):
        count = mesh.shape[axis]
        step = count // len(arrays)
        moved = [arrays[0]]
        for k in range(1, len(arrays)):
            pairs = [(i, i ^ (k * step)) for i in range(count)]
            moved.append(lax.ppermute(arrays[k], axis, pairs))
        return moved

    def local(species, coupling, symbol_x, symbol_y, symbol_z):
        fields, size_x, share_y, share_z = species.shape
        size_y, size_z = share_y * rows, share_z * cols
        share_kx, share_ky = size_x // rows, size_y // cols
        groups = LANES // share_z
        blocks = share_y // groups
        all_units = share_kx // groups
        units = [all_units * s // sum(SHARES) for s in SHARES]
        assert sum(units) == all_units
        firsts = [groups * sum(units[:q]) for q in range(n_chunk)]
        f32, bf16 = jnp.float32, jnp.bfloat16

        def limit(*shapes):
            total = sum(int(np.prod(shape)) * size for shape, size in shapes)
            return pltpu.CompilerParams(vmem_limit_bytes=total + SPARE)

        def cost(flops, moved):
            return pl.CostEstimate(flops=flops, bytes_accessed=moved, transcendentals=0)

        lines = jnp.transpose(species, (0, 2, 3, 1)).reshape(fields, share_y * share_z, size_x)

        chips = rows // 2
        tall = max(chips, 8)
        tables_x = []
        for pair in range(2):
            picked = [
                (chip * 2 + pair) * share_kx + kx for kx in range(share_kx) for chip in range(chips)
            ]
            tables_x += split_table(mode_table(size_x)[picked])
        table_x = jnp.asarray(np.concatenate(tables_x, axis=0))
        message_shapes = [
            jax.ShapeDtypeStruct((fields, 2 * share_y, u * LANES), f32)
            for u in units
            for _ in range(chips)
        ]

        def x_step(values, sent):
            own = sent is None
            sent = sent or []
            return pl.pallas_call(
                functools.partial(x_kernel, chips, units, groups, own),
                out_shape=message_shapes,
                in_specs=[HBM if own else VMEM, VMEM] + [VMEM] * len(sent),
                out_specs=[VMEM] * len(message_shapes),
                input_output_aliases={2 + i: i for i in range(len(sent))},
                scratch_shapes=[
                    pltpu.VMEM(
                        (fields, share_kx * chips // tall, blocks * tall, LANES), f32
                    )
                ]
                + [
                    pltpu.VMEM(lines.shape, f32),
                    pltpu.SemaphoreType.DMA((fields,)),
                ]
                * own,
                cost_estimate=cost(3 * lines.size * size_x, 8 * lines.size),
                compiler_params=limit((lines.shape, 24)),
                name="x_step",
            )(values, table_x, *sent)

        other = lax.ppermute(lines, "row", [(i, i ^ 1) for i in range(rows)])
        sent = x_step(other, x_step(lines, None))

        order = [
            peer * share_y + b * groups + t
            for peer in range(rows)
            for t in range(groups)
            for b in range(blocks)
        ]
        high, low = split_table(mode_table(size_y)[:, order])
        table_y = jnp.asarray(np.concatenate([high, low, high], axis=1))

        def y_step(arrays):
            lanes = arrays[0].shape[2]
            shape = jax.ShapeDtypeStruct((fields, share_ky, lanes), f32)
            return pl.pallas_call(
                functools.partial(y_kernel, chips, cols),
                out_shape=[shape] * cols,
                in_specs=[VMEM] * (chips + 1),
                out_specs=[VMEM] * cols,
                scratch_shapes=[pltpu.VMEM((fields, 2, size_y, lanes), bf16)],
                cost_estimate=cost(
                    6 * fields * size_y * size_y * lanes, 8 * fields * size_y * lanes
                ),
                compiler_params=limit(((fields, size_y, lanes), 24), (table_y.shape, 4)),
                name="y_step",
            )(*arrays, table_y)

        table_z = [jnp.asarray(t) for t in split_table(mode_table(size_z))]
        wide_shape = (3 * cols * LANES, groups * size_z)
        wide = pl.pallas_call(
            functools.partial(z_table_kernel, cols, groups),
            out_shape=jax.ShapeDtypeStruct(wide_shape, bf16),
            in_specs=[VMEM] * 2,
            out_specs=VMEM,
            compiler_params=limit((wide_shape, 2)),
            cost_estimate=cost(2 * size_z**3, 2 * int(np.prod(wide_shape))),
            name="z_table",
        )(*table_z)
        part_y = lax.dynamic_slice_in_dim(symbol_y, lax.axis_index("col") * share_ky, share_ky)
        syz = 1.0 + (part_y[:, None] + symbol_z[None, :])
        out_shape = jax.ShapeDtypeStruct((fields, share_kx, share_ky, size_z), f32)

        def z_step(q, arrays, prior):
            lanes = arrays[0].shape[2]
            has_prior = prior is not None
            return pl.pallas_call(
                functools.partial(z_kernel, cols, groups, firsts[q], has_prior),
                out_shape=out_shape,
                in_specs=[VMEM] * (cols + 2) + [SMEM] * 2 + [ANY] * has_prior,
                out_specs=ANY,
                input_output_aliases={cols + 4: 0} if has_prior else {},
                scratch_shapes=[
                    pltpu.VMEM((fields, units[q] * groups, share_ky, size_z), f32),
                    pltpu.SemaphoreType.DMA((units[q],)),
                ],
                cost_estimate=cost(
                    6 * fields * share_ky * lanes * cols * groups * size_z,
                    8 * cols * fields * share_ky * lanes,
                ),
                compiler_params=limit(
                    ((cols, fields, share_ky, lanes), 24), (wide_shape, 4)
                ),
                name="z_step",
            )(*arrays, wide, syz, symbol_x, coupling, *([prior] if has_prior else []))

        lines_z = []
        for q in range(n_chunk):
            received = exchange(sent[q * chips : (q + 1) * chips], "row")
            lines_z.append(exchange(y_step(received), "col"))
        modes = None
        for q in range(n_chunk):
            modes = z_step(q, lines_z[q], modes)
        return modes

    return jax.shard_map(
        local,
        mesh=mesh,
        in_specs=(P(None, None, "row", "col"), P(), P(), P(), P()),
        out_specs=P(None, "row", "col", None),
        check_vma=False,
    )
```

```python
import functools

import jax
import jax.numpy as jnp
import numpy as np
from jax import lax
from jax.experimental import pallas as pl
from jax.experimental.pallas import tpu as pltpu
from jax.sharding import PartitionSpec as P


LANES = 128
SPARE = 4 << 20
SHARES = (1, 2, 2, 3)


ANY = pl.BlockSpec(memory_space=pl.ANY)
VMEM = pl.BlockSpec(memory_space=pltpu.VMEM)


def mode_table(count):
    rank = np.arange(1, count + 1)
    angle = np.pi / (count + 1) * (rank[:, None] * rank[None, :] % (2 * count + 2))
    return np.sin(angle) * np.sqrt(2.0 / (count + 1))


def split_table(table):
    table = table.astype(np.float32)
    high = table.astype(jnp.bfloat16)
    low = (table - high.astype(np.float32)).astype(jnp.bfloat16)
    return high, low


def split(values):
    high = values.astype(jnp.bfloat16)
    low = (values - high.astype(jnp.float32)).astype(jnp.bfloat16)
    return high, low


def dot(a, b, contract):
    return lax.dot_general(
        a, b, ((contract[:1], contract[1:]), ((), ())), preferred_element_type=jnp.float32
    )


def block_transpose(tiles, width):
    count = len(tiles)
    lane = lax.broadcasted_iota(jnp.int32, tiles[0].shape, 1)
    step = count // 2
    while step:
        odd = (lane // (width * step)) % 2 == 1
        result = list(tiles)
        for g in range(count):
            if g & step:
                continue
            a, b = tiles[g], tiles[g + step]
            shift = width * step
            result[g] = jnp.where(odd, pltpu.roll(b, shift, 1), a)
            result[g + step] = jnp.where(odd, b, pltpu.roll(a, LANES - shift, 1))
        tiles = result
        step //= 2
    return tiles


def x_kernel(chips, units, groups, first, lines, table_ref, *refs):
    if not first:
        refs = refs[len(units) * chips :]
    outs, refs = refs[: len(units) * chips], refs[len(units) * chips :]
    scratch = refs[0]
    fields, rows, _ = lines.shape
    blocks = rows // LANES
    share_y = blocks * groups
    me = lax.axis_index("row")
    pair = me % 2
    owner = pair if first else 1 - pair
    depth = table_ref.shape[0] // 2
    table = table_ref[pl.ds(pl.multiple_of(pair * depth, depth), depth), :]
    half = depth // 2
    tall = scratch.shape[2] // blocks
    for f in range(fields):
        high, low = split(lines[f])
        both = dot(table, high, (1, 1))
        result = both[:half] + both[half:] + dot(table[:half], low, (1, 1))
        for j in range(half // tall):
            for b in range(blocks):
                scratch[f, j, b * tall : (b + 1) * tall, :] = result[
                    j * tall : (j + 1) * tall, b * LANES : (b + 1) * LANES
                ]
        start = 0
        for q, count in enumerate(units):
            for k in range(chips):
                chip = (me // 2) ^ k
                for hi in range(count):
                    tiles = []
                    for g in range(groups):
                        at = (start + hi * groups + g) * chips
                        place = pl.ds(at % tall + chip, blocks, stride=tall)
                        tiles.append(scratch[f, at // tall, place, :])
                    for t, tile in enumerate(block_transpose(tiles, LANES // groups)):
                        place = pl.ds(
                            pl.multiple_of(owner * share_y + t * blocks, blocks), blocks
                        )
                        outs[q * chips + k][f, place, hi * LANES : (hi + 1) * LANES] = tile
            start += count * groups


def y_kernel(peers, heads, *refs):
    ins, refs = refs[:peers], refs[peers:]
    table, outs, gathered = refs[0], refs[1 : 1 + heads], refs[1 + heads]
    fields, share = ins[0].shape[:2]
    out_share = outs[0].shape[1]
    chip, col = lax.axis_index("row") // 2, lax.axis_index("col")
    left = jnp.concatenate(
        [
            table[pl.ds(pl.multiple_of((col ^ k) * out_share, out_share), out_share), :]
            for k in range(heads)
        ],
        axis=0,
    )
    for f in range(fields):
        for k in range(peers):
            place = pl.ds(pl.multiple_of((chip ^ k) * share, share), share)
            high, low = split(ins[k][f])
            gathered[f, 0, place, :] = high
            gathered[f, 1, place, :] = low
    for f in range(fields):
        high, low = gathered[f, 0], gathered[f, 1]
        result = dot(left, jnp.concatenate([high, high, low], axis=0), (1, 0))
        for k in range(heads):
            outs[k][f] = result[k * out_share : (k + 1) * out_share]


def z_table_kernel(peers, groups, table_high, table_low, wide):
    depth, out_width = table_high.shape
    z_share = depth // peers
    col = lax.axis_index("col")
    wide[...] = jnp.zeros_like(wide)
    for part, table in enumerate((table_high, table_low, table_high)):
        for k in range(peers):
            piece = table[pl.ds(pl.multiple_of((col ^ k) * z_share, z_share), z_share), :]
            for g in range(groups):
                start = (part * peers + k) * LANES + g * z_share
                wide[start : start + z_share, g * out_width : (g + 1) * out_width] = piece


def z_kernel(peers, groups, first, has_prior, *refs):
    ins, refs = refs[:peers], refs[peers:]
    wide, syz, sx, coupling = refs[:4]
    modes, mixed, sems = refs[4 + has_prior :]
    fields, share, lanes = ins[0].shape
    units = lanes // LANES
    out_width = wide.shape[1] // groups
    parts = []
    for hi in range(units):
        for f in range(fields):
            block = jnp.concatenate(
                [ins[k][f, :, hi * LANES : (hi + 1) * LANES] for k in range(peers)], axis=1
            )
            high, low = split(block)
            parts.append(jnp.concatenate([high, high, low], axis=1))
    old = dot(jnp.concatenate(parts, axis=0), wide[...], (1, 0))
    stores = []
    for hi in range(units):
        for g in range(groups):
            kx = hi * groups + g
            weight = 1.0 / (syz[...] + sx[first + kx : first + kx + 1, :])
            rest = 1.0 - weight
            mine = [
                old[
                    (hi * fields + f) * share : (hi * fields + f + 1) * share,
                    g * out_width : (g + 1) * out_width,
                ]
                for f in range(fields)
            ]
            for a in range(fields):
                pair = [coupling[a * fields + b : a * fields + b + 1, :] for b in range(fields)]
                mix = pair[0] * mine[0]
                for b in range(1, fields):
                    mix = mix + pair[b] * mine[b]
                mixed[a, kx] = weight * mine[a] + rest * mix
        stores.append(
            pltpu.make_async_copy(
                mixed.at[:, hi * groups : (hi + 1) * groups],
                modes.at[:, pl.ds(first + hi * groups, groups)],
                sems.at[hi],
            )
        )
        stores[-1].start()
    for store in stores:
        store.wait()


def solution(mesh):
    rows, cols = mesh.shape["row"], mesh.shape["col"]
    n_chunk = len(SHARES)

    def exchange(arrays, axis):
        count = mesh.shape[axis]
        step = count // len(arrays)
        moved = [arrays[0]]
        for k in range(1, len(arrays)):
            pairs = [(i, i ^ (k * step)) for i in range(count)]
            moved.append(lax.ppermute(arrays[k], axis, pairs))
        return moved

    def local(species, coupling, symbol_x, symbol_y, symbol_z):
        fields, size_x, share_y, share_z = species.shape
        size_y, size_z = share_y * rows, share_z * cols
        share_kx, share_ky = size_x // rows, size_y // cols
        groups = LANES // share_z
        blocks = share_y // groups
        all_units = share_kx // groups
        units = [all_units * s // sum(SHARES) for s in SHARES]
        assert sum(units) == all_units
        firsts = [groups * sum(units[:q]) for q in range(n_chunk)]
        f32, bf16 = jnp.float32, jnp.bfloat16

        def limit(*shapes):
            total = sum(int(np.prod(shape)) * size for shape, size in shapes)
            return pltpu.CompilerParams(vmem_limit_bytes=total + SPARE)

        def cost(flops, moved):
            return pl.CostEstimate(flops=flops, bytes_accessed=moved, transcendentals=0)

        lines = jnp.transpose(species, (0, 2, 3, 1)).reshape(fields, share_y * share_z, size_x)

        chips = rows // 2
        tall = max(chips, 8)
        tables_x = []
        for pair in range(2):
            picked = [
                (chip * 2 + pair) * share_kx + kx for kx in range(share_kx) for chip in range(chips)
            ]
            tables_x += split_table(mode_table(size_x)[picked])
        table_x = jnp.asarray(np.concatenate(tables_x, axis=0))
        message_shapes = [
            jax.ShapeDtypeStruct((fields, 2 * share_y, u * LANES), f32)
            for u in units
            for _ in range(chips)
        ]

        def x_step(values, sent):
            own = sent is None
            sent = sent or []
            return pl.pallas_call(
                functools.partial(x_kernel, chips, units, groups, own),
                out_shape=message_shapes,
                in_specs=[VMEM] * (2 + len(sent)),
                out_specs=[VMEM] * len(message_shapes),
                input_output_aliases={2 + i: i for i in range(len(sent))},
                scratch_shapes=[
                    pltpu.VMEM(
                        (fields, share_kx * chips // tall, blocks * tall, LANES), f32
                    )
                ],
                cost_estimate=cost(3 * lines.size * size_x, 8 * lines.size),
                compiler_params=limit((lines.shape, 24)),
                name="x_step",
            )(values, table_x, *sent)

        other = lax.ppermute(lines, "row", [(i, i ^ 1) for i in range(rows)])
        sent = x_step(other, x_step(lines, None))

        order = [
            peer * share_y + b * groups + t
            for peer in range(rows)
            for t in range(groups)
            for b in range(blocks)
        ]
        high, low = split_table(mode_table(size_y)[:, order])
        table_y = jnp.asarray(np.concatenate([high, low, high], axis=1))

        def y_step(arrays):
            lanes = arrays[0].shape[2]
            shape = jax.ShapeDtypeStruct((fields, share_ky, lanes), f32)
            return pl.pallas_call(
                functools.partial(y_kernel, chips, cols),
                out_shape=[shape] * cols,
                in_specs=[VMEM] * (chips + 1),
                out_specs=[VMEM] * cols,
                scratch_shapes=[pltpu.VMEM((fields, 2, size_y, lanes), bf16)],
                cost_estimate=cost(
                    6 * fields * size_y * size_y * lanes, 8 * fields * size_y * lanes
                ),
                compiler_params=limit(((fields, size_y, lanes), 24), (table_y.shape, 4)),
                name="y_step",
            )(*arrays, table_y)

        table_z = [jnp.asarray(t) for t in split_table(mode_table(size_z))]
        wide_shape = (3 * cols * LANES, groups * size_z)
        wide = pl.pallas_call(
            functools.partial(z_table_kernel, cols, groups),
            out_shape=jax.ShapeDtypeStruct(wide_shape, bf16),
            in_specs=[VMEM] * 2,
            out_specs=VMEM,
            compiler_params=limit((wide_shape, 2)),
            cost_estimate=cost(2 * size_z**3, 2 * int(np.prod(wide_shape))),
            name="z_table",
        )(*table_z)
        part_y = lax.dynamic_slice_in_dim(symbol_y, lax.axis_index("col") * share_ky, share_ky)
        syz = 1.0 + (part_y[:, None] + symbol_z[None, :])
        part_x = lax.dynamic_slice_in_dim(symbol_x, lax.axis_index("row") * share_kx, share_kx)
        sx = jnp.broadcast_to(part_x[:, None], (share_kx, size_z))
        mix = jnp.broadcast_to(coupling.reshape(-1, 1), (fields * fields, size_z))
        out_shape = jax.ShapeDtypeStruct((fields, share_kx, share_ky, size_z), f32)

        def z_step(q, arrays, prior):
            lanes = arrays[0].shape[2]
            has_prior = prior is not None
            return pl.pallas_call(
                functools.partial(z_kernel, cols, groups, firsts[q], has_prior),
                out_shape=out_shape,
                in_specs=[VMEM] * (cols + 4) + [ANY] * has_prior,
                out_specs=ANY,
                input_output_aliases={cols + 4: 0} if has_prior else {},
                scratch_shapes=[
                    pltpu.VMEM((fields, units[q] * groups, share_ky, size_z), f32),
                    pltpu.SemaphoreType.DMA((units[q],)),
                ],
                cost_estimate=cost(
                    6 * fields * share_ky * lanes * cols * groups * size_z,
                    8 * cols * fields * share_ky * lanes,
                ),
                compiler_params=limit(
                    ((cols, fields, share_ky, lanes), 24), (wide_shape, 4)
                ),
                name="z_step",
            )(*arrays, wide, syz, sx, mix, *([prior] if has_prior else []))

        lines_z = []
        for q in range(n_chunk):
            received = exchange(sent[q * chips : (q + 1) * chips], "row")
            lines_z.append(exchange(y_step(received), "col"))
        modes = None
        for q in range(n_chunk):
            modes = z_step(q, lines_z[q], modes)
        return modes

    return jax.shard_map(
        local,
        mesh=mesh,
        in_specs=(P(None, None, "row", "col"), P(), P(), P(), P()),
        out_specs=P(None, "row", "col", None),
        check_vma=False,
    )
```
